32 devices in a mesh: vocab: 8 (over y, x, core), depth: 4 (over z).
Axes of the slice: x: 2, y: 2, z: 4, core: 2. Of those that a mesh axis runs over, the one named last changes fastest.
Arguments:
- states: bfloat16 [64, 4, 8192], P('vocab', 'depth'), may hold values from -400 to 400
- embedding: bfloat16 [152064, 8192], P(('vocab', 'depth')), may hold values from -1 to 1
- draft_ids: int32 [64, 4], P('vocab', 'depth'), may hold values from 0 to 152063
- target_ids: int32 [64, 4], P('vocab', 'depth'), may hold values from 0 to 152063
- lengths: int32 [64], P('vocab'), may hold values from 0 to 4
Outputs:
- target_logprob: float32 [64, 4], P('vocab', 'depth')
- draft_logprob: float32 [64, 4], P('vocab', 'depth')
- accepted_logprob: float32 [64], P('vocab')
The draws below stay inside these ranges and needn't reach their ends.
All inputs are finite; a program needn't handle non-finite values.
Results may differ from the reference program's by a relative error of at most 0.0003.
Values may be sent and summed in bfloat16 or wider, within the bound.
No kernel may reach another device: no remote copies, remote signals or barrier semaphores. Data moves between devices by JAX's collectives and lax.ppermute only.
A program may use at most 128 MiB of HBM per device.

```python
import jax
import jax.numpy as jnp
from jax import lax

D = 8192
VOCAB = 152064
DEPTHS = 4
SEQS = 64
N_VOCAB = 8
N_DEPTH = 4


def embed_row(key, index):
    values = jax.random.normal(jax.random.fold_in(jax.random.fold_in(key, 91), index), (D,), jnp.float32)
    return jnp.clip(values, -6.0, 6.0) / jnp.sqrt(jnp.float32(D))


def draw_embedding(key, part):
    rows = jnp.arange(VOCAB, dtype=jnp.int32)
    table = jax.vmap(lambda index: embed_row(key, index))(rows)
    return table.astype(jnp.bfloat16)


def drawn_rows(key, row_count):
    first_ids = jax.random.randint(jax.random.fold_in(key, 17), (row_count,), 0, VOCAB)
    offsets = jax.random.randint(jax.random.fold_in(key, 19), (row_count,), 1, VOCAB)
    second_ids = (first_ids + offsets) % VOCAB
    first_rows = jax.vmap(lambda index: embed_row(key, index))(first_ids).astype(jnp.bfloat16).astype(jnp.float32)
    second_rows = jax.vmap(lambda index: embed_row(key, index))(second_ids).astype(jnp.bfloat16).astype(jnp.float32)
    top_score = jax.random.uniform(jax.random.fold_in(key, 23), (row_count,), jnp.float32, 230.0, 310.0)
    gap = jax.random.uniform(jax.random.fold_in(key, 29), (row_count,), jnp.float32, 1.0, 3.0)
    second_score = top_score - gap
    gram_first = jnp.sum(first_rows * first_rows, axis=1)
    gram_second = jnp.sum(second_rows * second_rows, axis=1)
    gram_cross = jnp.sum(first_rows * second_rows, axis=1)
    determinant = gram_first * gram_second - gram_cross * gram_cross
    first_weight = (gram_second * top_score - gram_cross * second_score) / determinant
    second_weight = (gram_first * second_score - gram_cross * top_score) / determinant
    return first_weight[:, None] * first_rows + second_weight[:, None] * second_rows


def draw_states(key, part):
    row_count = SEQS * DEPTHS
    drawn = jnp.clip(3.0 * jax.random.normal(jax.random.fold_in(key, 5), (row_count, D), jnp.float32), -18.0, 18.0)
    aligned = drawn_rows(key, row_count)
    picked = jax.random.randint(jax.random.fold_in(key, 31), (row_count, 1), 0, 4) == 0
    values = jnp.clip(jnp.where(picked, aligned, drawn), -400.0, 400.0).reshape(SEQS, DEPTHS, D)
    return values.astype(jnp.bfloat16)


def touch_ends(array, key, low, high):
    index_at = [jax.random.randint(jax.random.fold_in(key, axis), (), 0, length) for axis, length in enumerate(array.shape)]
    longest = array.shape.index(max(array.shape))
    next_to = index_at[:longest] + [(index_at[longest] + 1) % array.shape[longest]] + index_at[longest + 1:]
    return array.at[tuple(index_at)].set(low).at[tuple(next_to)].set(high)


def setup_inputs(seed: int = 0) -> dict:
    arg_keys = jax.random.split(jax.random.key(seed), 6)
    states = draw_states(jax.random.fold_in(arg_keys[5], 71), 0)
    embedding = draw_embedding(jax.random.fold_in(arg_keys[5], 71), 0)
    draft_ids = touch_ends(jax.random.randint(arg_keys[2], (SEQS, DEPTHS), 0, VOCAB), jax.random.fold_in(arg_keys[2], 1), 0, VOCAB - 1).astype(jnp.int32)
    target_ids = touch_ends(jax.random.randint(arg_keys[3], (SEQS, DEPTHS), 0, VOCAB), jax.random.fold_in(arg_keys[3], 1), 0, VOCAB - 1).astype(jnp.int32)
    lengths = touch_ends(jax.random.randint(arg_keys[4], (SEQS,), 0, DEPTHS + 1), jax.random.fold_in(arg_keys[4], 1), 0, DEPTHS).astype(jnp.int32)
    return {"states": states, "embedding": embedding, "draft_ids": draft_ids, "target_ids": target_ids, "lengths": lengths}


def reference(states, embedding, draft_ids, target_ids, lengths):
    row_count = SEQS * DEPTHS
    flat = states.reshape(row_count, D)
    block_count = N_VOCAB * N_DEPTH
    block_size = VOCAB // block_count
    blocks = embedding.reshape(block_count, block_size, D)
    draft_flat = draft_ids.reshape(row_count, 1)
    target_flat = target_ids.reshape(row_count, 1)

    def step(carry, inputs):
        peak, total, target_sum, draft_sum = carry
        index, block = inputs
        logits = jnp.dot(flat, block.T, preferred_element_type=jnp.float32)
        columns = (lax.iota(jnp.int32, block_size) + index * block_size)[None, :]
        new_peak = jnp.maximum(peak, jnp.max(logits, axis=1))
        total = total * jnp.exp(peak - new_peak) + jnp.sum(jnp.exp(logits - new_peak[:, None]), axis=1)
        target_sum = target_sum + jnp.sum(jnp.where(columns == target_flat, logits, jnp.float32(0.0)), axis=1)
        draft_sum = draft_sum + jnp.sum(jnp.where(columns == draft_flat, logits, jnp.float32(0.0)), axis=1)
        return (new_peak, total, target_sum, draft_sum), None

    start = (jnp.full((row_count,), -1e30, jnp.float32), jnp.zeros((row_count,), jnp.float32),
             jnp.zeros((row_count,), jnp.float32), jnp.zeros((row_count,), jnp.float32))
    (peak, total, target_sum, draft_sum), unused = lax.scan(step, start, (jnp.arange(block_count, dtype=jnp.int32), blocks))
    lse = peak + jnp.log(total)
    target_logprob = (target_sum - lse).reshape(SEQS, DEPTHS)
    draft_logprob = (draft_sum - lse).reshape(SEQS, DEPTHS)
    depth_index = jnp.arange(DEPTHS, dtype=jnp.int32)[None, :]
    accepted_logprob = jnp.sum(jnp.where(depth_index < lengths[:, None], draft_logprob, jnp.float32(0.0)), axis=1)
    return target_logprob, draft_logprob, accepted_logprob
```

```python
import functools

import jax
import jax.numpy as jnp
from jax import lax
from jax.experimental import pallas as pl
from jax.experimental.pallas import tpu as pltpu
from jax.sharding import PartitionSpec as P

AXES = ("vocab", "depth")
ID_LANES = 128
LOW = -1e30
CHUNKS = 2


def xor_pairs(count, mask):
    return [(i, i ^ mask) for i in range(count)]


def parity_pairs(count, even_mask, odd_mask):
    return [(i, i ^ (odd_mask if i % 2 else even_mask)) for i in range(count)]


def stage_masks(vocab_count):
    bits = [1 << b for b in range(1, vocab_count.bit_length() - 1)]
    return list(reversed(bits)), bits


def block_mask(masks, position):
    mask = 0
    for stage, stage_mask in enumerate(masks):
        if position >> stage & 1:
            mask ^= stage_mask
    return mask


def block_rows(shard_rows):
    best = 0
    for rows in range(256, 641, 16):
        if shard_rows % rows == 0:
            best = rows
    if best:
        return best
    steps = -(-shard_rows // 512)
    return -(-(-(-shard_rows // steps)) // 16) * 16


def gather_depth(own, depth_count):
    parts = [own] + [
        lax.ppermute(own, "depth", xor_pairs(depth_count, s)) for s in range(1, depth_count)
    ]
    return jnp.concatenate(parts, axis=0)


def assemble(pieces, held, masks_even, masks_odd, block, width):
    me = lax.axis_index("vocab")
    core = me % 2
    stages = len(masks_even)
    per_piece = 1 << (stages - 1)
    for number, piece in enumerate(pieces):
        from_partner = number // 2
        for place in range(per_piece):
            position = place + (number % 2) * per_piece
            even, odd = block_mask(masks_even, position), block_mask(masks_odd, position)
            source_core = core ^ 1 if from_partner else core
            mask = jnp.where(source_core == 1, odd, even)
            source = (me ^ 1 if from_partner else me) ^ mask
            start = pl.multiple_of(source * block, block)
            held[pl.ds(start, block), :] = piece[pl.ds(place * block, block), :]


def dot_nt(a, b):
    return lax.dot_general(a, b, (((1,), (1,)), ((), ())), preferred_element_type=jnp.float32)


def partial_kernel(geometry, e_ref, *refs):
    pieces, out_ref, held = refs[:-2], refs[-2], refs[-1]
    masks_even, masks_odd, block, width = geometry

    @pl.when(pl.program_id(0) == 0)
    def _():
        assemble(pieces, held, masks_even, masks_odd, block, width)

    out_ref[...] = dot_nt(e_ref[...], held[...])


def fold(values, base, limit, peak, total, target, draft, ids):
    rows, lanes = values.shape
    groups = rows // 8
    tiles = values.reshape(groups, 8, lanes)
    number = base + (
        lax.broadcasted_iota(jnp.int32, (groups, 8, lanes), 0) * 8
        + lax.broadcasted_iota(jnp.int32, (groups, 8, lanes), 1)
    )
    if limit is not None:
        tiles = jnp.where(number < limit, tiles, LOW)
    new_peak = jnp.maximum(peak[...], jnp.max(tiles, axis=0))
    total[...] = total[...] * jnp.exp(peak[...] - new_peak) + jnp.sum(
        jnp.exp(tiles - new_peak[None]), axis=0
    )
    target[...] += jnp.sum(jnp.where(number == ids[0:8][None], tiles, 0.0), axis=0)
    draft[...] += jnp.sum(jnp.where(number == ids[8:16][None], tiles, 0.0), axis=0)
    peak[...] = new_peak


def final_kernel(geometry, sizes, has_partial, e_ref, *refs):
    masks_even, masks_odd, block, width = geometry
    steps, rows, shard_rows, vocab_count, depth_count = sizes
    scratch = refs[-8:]
    held, logits, peak, total, target, draft, ids, packed = scratch
    out_ref = refs[-9]
    pieces = refs[:-9]
    partial_ref = None
    if has_partial:
        partial_ref, pieces = pieces[0], pieces[1:]
    step = pl.program_id(0)
    limit = None if steps * rows == shard_rows else shard_rows
    lanes = peak.shape[1]

    @pl.when(step == 0)
    def _():
        assemble(pieces, held, masks_even, masks_odd, block, width)
        rank = lax.axis_index("vocab") * depth_count + lax.axis_index("depth")
        pick = (
            lax.broadcasted_iota(jnp.int32, (16, ID_LANES), 0)
            == lax.broadcasted_iota(jnp.int32, (16, ID_LANES), 1)
        )
        digits = dot_nt(
            jnp.where(pick, 1.0, 0.0).astype(jnp.bfloat16), held[:, width : width + ID_LANES]
        )
        wanted = digits[0:2] * 65536.0 + digits[2:4] * 256.0 + digits[4:6]
        wanted = wanted.astype(jnp.int32) - rank * shard_rows
        ids[0:8, :] = jnp.broadcast_to(wanted[0:1], (8, lanes))
        ids[8:16, :] = jnp.broadcast_to(wanted[1:2], (8, lanes))
        peak[...] = jnp.full_like(peak, LOW)
        total[...] = jnp.zeros_like(total)
        target[...] = jnp.zeros_like(target)
        draft[...] = jnp.zeros_like(draft)

    @pl.when(step > 0)
    def _():
        fold(
            logits[...], (step - 1) * rows, limit, peak, total, target, draft, ids
        )

    fresh = dot_nt(e_ref[...], held[:, 0:width])
    if has_partial:
        fresh = fresh + partial_ref[...]
    logits[...] = fresh

    @pl.when(step == steps - 1)
    def _():
        fold(logits[...], step * rows, limit, peak, total, target, draft, ids)
        top = jnp.max(peak[...], axis=0, keepdims=True)
        packed[...] = jnp.zeros_like(packed)
        packed[0:1, :] = top
        packed[1:2, :] = jnp.sum(total[...] * jnp.exp(peak[...] - top), axis=0, keepdims=True)
        packed[2:3, :] = jnp.sum(target[...], axis=0, keepdims=True)
        packed[3:4, :] = jnp.sum(draft[...], axis=0, keepdims=True)
        table = packed[...]
        own = block // depth_count
        lane = lax.broadcasted_iota(jnp.int32, table.shape, 1)
        depth = lax.axis_index("depth")
        bit = 1
        while bit < depth_count:
            reach = bit * own
            swapped = jnp.where(
                (lane // reach) % 2 == 0,
                pltpu.roll(table, lanes - reach, 1),
                pltpu.roll(table, reach, 1),
            )
            table = jnp.where((depth // bit) % 2 == 1, swapped, table)
            bit *= 2
        packed[...] = table
        for group in range(vocab_count):
            tile = packed[:, group * block : (group + 1) * block]
            row = jnp.concatenate([tile[k : k + 1] for k in range(4)], axis=1)
            out_ref[group * depth_count : (group + 1) * depth_count, :] = jnp.broadcast_to(
                row, (depth_count, 4 * block)
            )


def tail_kernel(sizes, all_ref, lengths_ref, target_ref, draft_ref, accepted_ref, lse_ref):
    own, depth_count, block = sizes
    table = all_ref[...]
    peaks = table[:, 0:block]
    top = jnp.max(peaks, axis=0, keepdims=True)
    total = jnp.sum(table[:, 1 * block : 2 * block] * jnp.exp(peaks - top), axis=0, keepdims=True)
    lse = top + jnp.log(total)
    lse_ref[0:1, 0:block] = jnp.sum(table[:, 2 * block : 3 * block], axis=0, keepdims=True) - lse
    lse_ref[1:2, 0:block] = jnp.sum(table[:, 3 * block : 4 * block], axis=0, keepdims=True) - lse
    depth = lax.axis_index("depth")
    target = jnp.zeros((1, own), jnp.float32)
    draft = jnp.zeros((1, own), jnp.float32)
    accepted = jnp.zeros((1, own), jnp.float32)
    lengths = lengths_ref[...]
    for d in range(depth_count):
        t = lse_ref[0:1, d * own : (d + 1) * own]
        g = lse_ref[1:2, d * own : (d + 1) * own]
        target = jnp.where(depth == d, t, target)
        draft = jnp.where(depth == d, g, draft)
        accepted = accepted + jnp.where(lengths > d, g, 0.0)
    target_ref[...] = target
    draft_ref[...] = draft
    accepted_ref[...] = accepted


def body(states, embedding, draft_ids, target_ids, lengths):
    seq_dev, depth_dev, model_width = states.shape
    own = seq_dev * depth_dev
    vocab_count, depth_count = lax.axis_size("vocab"), lax.axis_size("depth")
    block = own * depth_count
    lanes = block * vocab_count
    shard_rows = embedding.shape[0]
    own_rows = states.reshape(own, model_width)
    masks_even, masks_odd = stage_masks(vocab_count)

    pair = jnp.concatenate([target_ids.reshape(own, 1), draft_ids.reshape(own, 1)], axis=1)
    digits = jnp.concatenate([pair >> 16, (pair >> 8) & 255, pair & 255], axis=1)
    digits = jnp.pad(digits, ((0, 0), (0, ID_LANES - digits.shape[1]))).astype(jnp.bfloat16)

    def to_partner(x):
        return lax.ppermute(x, "vocab", xor_pairs(vocab_count, 1))

    width = model_width // CHUNKS
    gathered = []
    for chunk in range(CHUNKS):
        part = own_rows[:, chunk * width : (chunk + 1) * width]
        if chunk == CHUNKS - 1:
            part = jnp.concatenate([part, digits], axis=1)
        held = gather_depth(part, depth_count)
        for stage in range(len(masks_even)):
            moved = lax.ppermute(
                held, "vocab", parity_pairs(vocab_count, masks_even[stage], masks_odd[stage])
            )
            if stage < len(masks_even) - 1:
                held = jnp.concatenate([held, moved], axis=0)
        gathered.append((held, moved, to_partner(held), to_partner(moved)))

    rows = block_rows(shard_rows)
    steps = -(-shard_rows // rows)
    partial = None
    for chunk in range(CHUNKS):
        last = chunk == CHUNKS - 1
        geometry = (masks_even, masks_odd, block, width)
        pieces = gathered[chunk]
        held_width = width + (ID_LANES if last else 0)
        piece_specs = [
            pl.BlockSpec(p.shape, lambda i: (0, 0), pipeline_mode=pl.Buffered(1)) for p in pieces
        ]
        e_spec = pl.BlockSpec((rows, width), lambda i, c=chunk: (i, c))
        tile_spec = pl.BlockSpec((rows, lanes), lambda i: (i, 0))
        cost = pl.CostEstimate(
            flops=2 * shard_rows * lanes * width,
            bytes_accessed=2 * shard_rows * width,
            transcendentals=0,
        )
        held_scratch = pltpu.VMEM((lanes, held_width), jnp.bfloat16)
        if not last:
            partial = pl.pallas_call(
                functools.partial(partial_kernel, geometry),
                grid=(steps,),
                in_specs=[e_spec] + piece_specs,
                out_specs=tile_spec,
                out_shape=jax.ShapeDtypeStruct((shard_rows, lanes), jnp.float32),
                scratch_shapes=[held_scratch],
                compiler_params=pltpu.CompilerParams(vmem_limit_bytes=VMEM_LIMIT),
                cost_estimate=cost,
                name="partial_logits",
            )(embedding, *pieces)
        else:
            stat = pltpu.VMEM((8, lanes), jnp.float32)
            sizes = (steps, rows, shard_rows, vocab_count, depth_count)
            table = pl.pallas_call(
                functools.partial(final_kernel, geometry, sizes, partial is not None),
                grid=(steps,),
                in_specs=[e_spec] + ([tile_spec] if partial is not None else []) + piece_specs,
                out_specs=pl.BlockSpec((vocab_count * depth_count, 4 * block), lambda i: (0, 0)),
                out_shape=jax.ShapeDtypeStruct(
                    (vocab_count * depth_count, 4 * block), jnp.float32
                ),
                scratch_shapes=[
                    held_scratch,
                    pltpu.VMEM((rows, lanes), jnp.float32),
                    stat,
                    stat,
                    stat,
                    stat,
                    pltpu.VMEM((16, lanes), jnp.int32),
                    stat,
                ],
                compiler_params=pltpu.CompilerParams(vmem_limit_bytes=VMEM_LIMIT),
                cost_estimate=cost,
                name="final_logits",
            )(embedding, *([partial] if partial is not None else []), *pieces)

    shares = lax.all_to_all(table, AXES, 0, 0, tiled=True)
    line = jax.ShapeDtypeStruct((1, own), jnp.float32)
    target, draft, accepted = pl.pallas_call(
        functools.partial(tail_kernel, (own, depth_count, block)),
        out_shape=[line, line, line],
        scratch_shapes=[pltpu.VMEM((8, ID_LANES), jnp.float32)],
        name="combine",
    )(shares, lengths.reshape(1, own))
    shape = (seq_dev, depth_dev)
    return target.reshape(shape), draft.reshape(shape), accepted.reshape(seq_dev)


VMEM_LIMIT = 40 * 2**20


def solution(mesh):
    placed = (
        P("vocab", "depth", None),
        P(("vocab", "depth"), None),
        P("vocab", "depth"),
        P("vocab", "depth"),
        P("vocab"),
    )
    return jax.shard_map(
        body,
        mesh=mesh,
        in_specs=placed,
        out_specs=(P("vocab", "depth"), P("vocab", "depth"), P("vocab")),
        check_vma=False,
    )
```

```python
import functools

import jax
import jax.numpy as jnp
from jax import lax
from jax.experimental import pallas as pl
from jax.experimental.pallas import tpu as pltpu
from jax.sharding import PartitionSpec as P

AXES = ("vocab", "depth")
ID_LANES = 128
LOW = -1e30
CHUNKS = 2
DEPTH = 3
FIRST_PART = 12


def xor_pairs(count, mask):
    return [(i, i ^ mask) for i in range(count)]


def parity_pairs(count, even_mask, odd_mask):
    return [(i, i ^ (odd_mask if i % 2 else even_mask)) for i in range(count)]


def stage_masks(vocab_count):
    bits = [1 << b for b in range(1, vocab_count.bit_length() - 1)]
    return list(reversed(bits)), bits


def block_mask(masks, position):
    mask = 0
    for stage, stage_mask in enumerate(masks):
        if position >> stage & 1:
            mask ^= stage_mask
    return mask


def block_rows(shard_rows):
    best = 0
    for rows in range(256, 641, 16):
        if shard_rows % rows == 0:
            best = rows
    if best:
        return best
    steps = -(-shard_rows // 512)
    return -(-(-(-shard_rows // steps)) // 16) * 16


def gather_depth(own, depth_count):
    shifts = sorted(range(1, depth_count), key=lambda s: min(s, depth_count - s))
    parts = {0: own}
    for s in shifts:
        pairs = [(i, (i + s) % depth_count) for i in range(depth_count)]
        parts[depth_count - s] = lax.ppermute(own, "depth", pairs)
    return jnp.concatenate([parts[p] for p in range(depth_count)], axis=0)


def assemble(pieces, held, masks_even, masks_odd, block, width):
    me = lax.axis_index("vocab")
    core = me % 2
    stages = len(masks_even)
    per_piece = 1 << (stages - 1)
    for number, piece in enumerate(pieces):
        from_partner = number // 2
        for place in range(per_piece):
            position = place + (number % 2) * per_piece
            even, odd = block_mask(masks_even, position), block_mask(masks_odd, position)
            source_core = core ^ 1 if from_partner else core
            mask = jnp.where(source_core == 1, odd, even)
            source = (me ^ 1 if from_partner else me) ^ mask
            start = pl.multiple_of(source * block, block)
            held[pl.ds(start, block), :] = piece[pl.ds(place * block, block), :]


def dot_nt(a, b):
    return lax.dot_general(a, b, (((1,), (1,)), ((), ())), preferred_element_type=jnp.float32)


class Stream:
    def __init__(self, column, steps, e_ref, buffers, sems):
        self.column, self.steps = column, steps
        self.e_ref, self.buffers, self.sems = e_ref, buffers, sems
        self.depth, self.rows, self.width = buffers.shape

    def copy(self, step, slot):
        start = step * self.rows
        if not isinstance(step, int):
            start = pl.multiple_of(start, self.rows)
        return pltpu.make_async_copy(
            self.e_ref.at[pl.ds(start, self.rows), pl.ds(self.column, self.width)],
            self.buffers.at[slot],
            self.sems.at[slot],
        )

    def open(self):
        for step in range(min(self.depth, self.steps)):
            self.copy(step, step).start()

    def take(self, step):
        slot = lax.rem(step, self.depth)
        self.copy(step, slot).wait()
        return self.buffers.at[slot]

    def give_back(self, step):
        @pl.when(step + self.depth < self.steps)
        def _():
            self.copy(step + self.depth, lax.rem(step, self.depth)).start()


def partial_kernel(geometry, stream, e_ref, *refs):
    masks_even, masks_odd, block, width = geometry
    if stream is not None:
        stream, refs = Stream(*stream, e_ref, *refs[-2:]), refs[:-2]
    pieces, out_ref, held = refs[:-2], refs[-2], refs[-1]
    step = pl.program_id(0)

    @pl.when(step == 0)
    def _():
        if stream is not None:
            stream.open()
        assemble(pieces, held, masks_even, masks_odd, block, width)

    tile = e_ref if stream is None else stream.take(step)
    out_ref[...] = dot_nt(tile[...], held[...])
    if stream is not None:
        stream.give_back(step)


def fold(values, base, limit, peak, total, target, draft, ids):
    rows, lanes = values.shape
    groups = rows // 8
    tiles = values.reshape(groups, 8, lanes)
    number = base + (
        lax.broadcasted_iota(jnp.int32, (groups, 8, lanes), 0) * 8
        + lax.broadcasted_iota(jnp.int32, (groups, 8, lanes), 1)
    )
    if limit is not None:
        tiles = jnp.where(number < limit, tiles, LOW)
    new_peak = jnp.maximum(peak[...], jnp.max(tiles, axis=0))
    total[...] = total[...] * jnp.exp(peak[...] - new_peak) + jnp.sum(
        jnp.exp(tiles - new_peak[None]), axis=0
    )
    target[...] += jnp.sum(jnp.where(number == ids[0:8][None], tiles, 0.0), axis=0)
    draft[...] += jnp.sum(jnp.where(number == ids[8:16][None], tiles, 0.0), axis=0)
    peak[...] = new_peak


def final_kernel(geometry, sizes, has_partial, stream, e_ref, *refs):
    if stream is not None:
        stream, refs = Stream(*stream, e_ref, *refs[-2:]), refs[:-2]
    masks_even, masks_odd, block, width = geometry
    steps, rows, shard_rows, vocab_count, depth_count = sizes
    scratch = refs[-8:]
    held, logits, peak, total, target, draft, ids, packed = scratch
    out_ref = refs[-9]
    pieces = refs[:-9]
    partial_ref = None
    if has_partial:
        partial_ref, pieces = pieces[0], pieces[1:]
    step = pl.program_id(0)
    limit = None if steps * rows == shard_rows else shard_rows
    lanes = peak.shape[1]

    @pl.when(step == 0)
    def _():
        if stream is not None:
            stream.open()
        assemble(pieces, held, masks_even, masks_odd, block, width)
        rank = lax.axis_index("vocab") * depth_count + lax.axis_index("depth")
        pick = (
            lax.broadcasted_iota(jnp.int32, (16, ID_LANES), 0)
            == lax.broadcasted_iota(jnp.int32, (16, ID_LANES), 1)
        )
        digits = dot_nt(
            jnp.where(pick, 1.0, 0.0).astype(jnp.bfloat16), held[:, width : width + ID_LANES]
        )
        wanted = digits[0:2] * 65536.0 + digits[2:4] * 256.0 + digits[4:6]
        wanted = wanted.astype(jnp.int32) - rank * shard_rows
        wanted = jnp.where((wanted >= 0) & (wanted < shard_rows), wanted, -shard_rows - rows)
        ids[0:8, :] = jnp.broadcast_to(wanted[0:1], (8, lanes))
        ids[8:16, :] = jnp.broadcast_to(wanted[1:2], (8, lanes))
        logits[...] = jnp.full_like(logits, LOW)
        peak[...] = jnp.full_like(peak, LOW)
        total[...] = jnp.zeros_like(total)
        target[...] = jnp.zeros_like(target)
        draft[...] = jnp.zeros_like(draft)

    tile = e_ref if stream is None else stream.take(step)
    fold(logits[...], (step - 1) * rows, limit, peak, total, target, draft, ids)
    fresh = dot_nt(tile[...], held[:, 0:width])
    if has_partial:
        fresh = fresh + partial_ref[...]
    logits[...] = fresh
    if stream is not None:
        stream.give_back(step)

    @pl.when(step == steps - 1)
    def _():
        fold(logits[...], step * rows, limit, peak, total, target, draft, ids)
        top = jnp.max(peak[...], axis=0, keepdims=True)
        packed[...] = jnp.zeros_like(packed)
        packed[0:1, :] = top
        packed[1:2, :] = jnp.sum(total[...] * jnp.exp(peak[...] - top), axis=0, keepdims=True)
        packed[2:3, :] = jnp.sum(target[...], axis=0, keepdims=True)
        packed[3:4, :] = jnp.sum(draft[...], axis=0, keepdims=True)
        table = packed[...]
        own = block // depth_count
        lane = lax.broadcasted_iota(jnp.int32, table.shape, 1)
        depth = lax.axis_index("depth")
        place = lane % block
        bit = 1
        while bit < depth_count:
            reach = bit * own
            turned = jnp.where(
                place >= reach,
                pltpu.roll(table, reach, 1),
                pltpu.roll(table, lanes - (block - reach), 1),
            )
            table = jnp.where((depth // bit) % 2 == 1, turned, table)
            bit *= 2
        packed[...] = table
        for group in range(vocab_count):
            tile = packed[:, group * block : (group + 1) * block]
            row = jnp.concatenate([tile[k : k + 1] for k in range(4)], axis=1)
            out_ref[group * depth_count : (group + 1) * depth_count, :] = jnp.broadcast_to(
                row, (depth_count, 4 * block)
            )


def tail_kernel(sizes, all_ref, lengths_ref, target_ref, draft_ref, accepted_ref, lse_ref):
    own, depth_count, block = sizes
    table = all_ref[...]
    peaks = table[:, 0:block]
    top = jnp.max(peaks, axis=0, keepdims=True)
    total = jnp.sum(table[:, 1 * block : 2 * block] * jnp.exp(peaks - top), axis=0, keepdims=True)
    lse = top + jnp.log(total)
    lse_ref[0:1, 0:block] = jnp.sum(table[:, 2 * block : 3 * block], axis=0, keepdims=True) - lse
    lse_ref[1:2, 0:block] = jnp.sum(table[:, 3 * block : 4 * block], axis=0, keepdims=True) - lse
    depth = lax.axis_index("depth")
    target = jnp.zeros((1, own), jnp.float32)
    draft = jnp.zeros((1, own), jnp.float32)
    accepted = jnp.zeros((1, own), jnp.float32)
    lengths = lengths_ref[...]
    for d in range(depth_count):
        t = lse_ref[0:1, d * own : (d + 1) * own]
        g = lse_ref[1:2, d * own : (d + 1) * own]
        target = jnp.where(depth == d, t, target)
        draft = jnp.where(depth == d, g, draft)
        accepted = accepted + jnp.where(lengths > d, g, 0.0)
    target_ref[...] = target
    draft_ref[...] = draft
    accepted_ref[...] = accepted


def body(states, embedding, draft_ids, target_ids, lengths):
    seq_dev, depth_dev, model_width = states.shape
    own = seq_dev * depth_dev
    vocab_count, depth_count = lax.axis_size("vocab"), lax.axis_size("depth")
    block = own * depth_count
    lanes = block * vocab_count
    shard_rows = embedding.shape[0]
    own_rows = states.reshape(own, model_width)
    masks_even, masks_odd = stage_masks(vocab_count)

    pair = jnp.concatenate([target_ids.reshape(own, 1), draft_ids.reshape(own, 1)], axis=1)
    digits = jnp.concatenate([pair >> 16, (pair >> 8) & 255, pair & 255], axis=1)
    digits = jnp.pad(digits, ((0, 0), (0, ID_LANES - digits.shape[1]))).astype(jnp.bfloat16)

    def to_partner(x):
        return lax.ppermute(x, "vocab", xor_pairs(vocab_count, 1))

    first = model_width * FIRST_PART // 32 // 256 * 256
    widths = [first, model_width - first]
    starts = [0, first]
    gathered = []
    for chunk in range(CHUNKS):
        part = own_rows[:, starts[chunk] : starts[chunk] + widths[chunk]]
        if chunk == CHUNKS - 1:
            part = jnp.concatenate([part, digits], axis=1)
        held = gather_depth(part, depth_count)
        for stage in range(len(masks_even)):
            moved = lax.ppermute(
                held, "vocab", parity_pairs(vocab_count, masks_even[stage], masks_odd[stage])
            )
            if stage < len(masks_even) - 1:
                held = jnp.concatenate([held, moved], axis=0)
        gathered.append([held, moved, to_partner(held)])

    rows = block_rows(shard_rows)
    steps = -(-shard_rows // rows)
    partial = None
    for chunk in range(CHUNKS):
        last = chunk == CHUNKS - 1
        width = widths[chunk]
        geometry = (masks_even, masks_odd, block, width)
        pieces = gathered[chunk]
        if partial is not None:
            pieces[1], partial = lax.optimization_barrier((pieces[1], partial))
        pieces = pieces + [to_partner(pieces[1])]
        held_width = width + (ID_LANES if last else 0)
        piece_specs = [
            pl.BlockSpec(p.shape, lambda i: (0, 0), pipeline_mode=pl.Buffered(1)) for p in pieces
        ]
        streamed = steps * rows == shard_rows
        if streamed:
            e_spec = pl.BlockSpec(memory_space=pl.ANY)
            stream = (starts[chunk], steps)
            slots = [
                pltpu.VMEM((DEPTH, rows, width), jnp.bfloat16),
                pltpu.SemaphoreType.DMA((DEPTH,)),
            ]
        else:
            e_spec = pl.BlockSpec(
                (pl.Element(rows, (0, steps * rows - shard_rows)), pl.Element(width)),
                lambda i, c=starts[chunk]: (i * rows, c),
            )
            stream, slots = None, []
        tile_spec = pl.BlockSpec((rows, lanes), lambda i: (i, 0))
        cost = pl.CostEstimate(
            flops=2 * shard_rows * lanes * width,
            bytes_accessed=2 * shard_rows * width,
            transcendentals=0,
        )
        held_scratch = pltpu.VMEM((lanes, held_width), jnp.bfloat16)
        if not last:
            partial = pl.pallas_call(
                functools.partial(partial_kernel, geometry, stream),
                grid=(steps,),
                in_specs=[e_spec] + piece_specs,
                out_specs=tile_spec,
                out_shape=jax.ShapeDtypeStruct((shard_rows, lanes), jnp.float32),
                scratch_shapes=[held_scratch] + slots,
                compiler_params=pltpu.CompilerParams(vmem_limit_bytes=VMEM_LIMIT),
                cost_estimate=cost,
                name="partial_logits",
            )(embedding, *pieces)
        else:
            stat = pltpu.VMEM((8, lanes), jnp.float32)
            sizes = (steps, rows, shard_rows, vocab_count, depth_count)
            table = pl.pallas_call(
                functools.partial(final_kernel, geometry, sizes, partial is not None, stream),
                grid=(steps,),
                in_specs=[e_spec] + ([tile_spec] if partial is not None else []) + piece_specs,
                out_specs=pl.BlockSpec((vocab_count * depth_count, 4 * block), lambda i: (0, 0)),
                out_shape=jax.ShapeDtypeStruct(
                    (vocab_count * depth_count, 4 * block), jnp.float32
                ),
                scratch_shapes=[
                    held_scratch,
                    pltpu.VMEM((rows, lanes), jnp.float32),
                    stat,
                    stat,
                    stat,
                    stat,
                    pltpu.VMEM((16, lanes), jnp.int32),
                    stat,
                ]
                + slots,
                compiler_params=pltpu.CompilerParams(vmem_limit_bytes=VMEM_LIMIT),
                cost_estimate=cost,
                name="final_logits",
            )(embedding, *([partial] if partial is not None else []), *pieces)

    shares = lax.all_to_all(table, AXES, 0, 0, tiled=True)
    line = jax.ShapeDtypeStruct((1, own), jnp.float32)
    target, draft, accepted = pl.pallas_call(
        functools.partial(tail_kernel, (own, depth_count, block)),
        out_shape=[line, line, line],
        scratch_shapes=[pltpu.VMEM((8, ID_LANES), jnp.float32)],
        name="combine",
    )(shares, lengths.reshape(1, own))
    shape = (seq_dev, depth_dev)
    return target.reshape(shape), draft.reshape(shape), accepted.reshape(seq_dev)


VMEM_LIMIT = 44 * 2**20


def solution(mesh):
    placed = (
        P("vocab", "depth", None),
        P(("vocab", "depth"), None),
        P("vocab", "depth"),
        P("vocab", "depth"),
        P("vocab"),
    )
    return jax.shard_map(
        body,
        mesh=mesh,
        in_specs=placed,
        out_specs=(P("vocab", "depth"), P("vocab", "depth"), P("vocab")),
        check_vma=False,
    )
```
